32 devices in a mesh: ta: 4 (over z), sa: 8 (over y, x, core).
Axes of the slice: x: 2, y: 2, z: 4, core: 2. Of those that a mesh axis runs over, the one named last changes fastest.
Arguments:
- frames: float32 [16, 8, 512, 4096], P('ta', 'sa'), may hold values from -6 to 6
- taps: float32 [7], replicated, may hold values from 0.1 to 0.3
Outputs:
- columns: float32 [64, 16, 512, 512], P('sa', 'ta')
The draws below stay inside these ranges and needn't reach their ends.
All inputs are finite; a program needn't handle non-finite values.
Results may differ from the reference program's by a relative error of at most 0.00002.
Values sent between devices are 32-bit elements; how exact they have to be, the bound alone decides.
A program may use at most 256 MiB of HBM per device.

```python
import jax
import jax.numpy as jnp
from jax import lax

NY = 4096
NX = 4096
TS = 512
TIME = 16
READERS = 8
STRIP = 512
TILES = 64
N_SA = 8


def level_of(rng, extent, cuts, low, high):
    gain = 1.0
    for axis_at, blocks in cuts:
        heights = jax.random.uniform(jax.random.fold_in(jax.random.fold_in(rng, 6), axis_at), (blocks,), jnp.float32, low / len(cuts), high / len(cuts))
        gain = gain * jnp.repeat(jnp.exp(heights), extent[axis_at] // blocks).reshape((-1,) + (1,) * (len(extent) - 1 - axis_at))
    return gain


def normal_values(stream_key, shape, deviation, limit, pieces=(), kind=jnp.bfloat16):
    result = deviation * jax.random.normal(stream_key, shape, jnp.float32)
    if pieces:
        result = result * level_of(stream_key, shape, pieces, -0.22, 0.18)
    return jnp.clip(result, -limit, limit).astype(kind)


def setup_inputs(seed: int = 0) -> dict:
    seeds = jax.random.split(jax.random.key(seed), 3)
    return {
        "frames": normal_values(seeds[0], (TIME, READERS, STRIP, NX), 1.0, 6.0, ((0, 4), (1, 8)), jnp.float32),
        "taps": jnp.clip(jax.random.uniform(seeds[1], (7,), jnp.float32, 0.1, 0.3), 0.1, 0.3),
    }


def reference(frames, taps):
    per_tile = TS // N_SA
    tile_rows = NY // TS
    tile_cols = NX // TS

    def one_row(index):
        piece = lax.dynamic_slice_in_dim(frames, index * per_tile, per_tile, 2)
        field = piece.transpose(0, 2, 1, 3).reshape(TIME, TS, NX)
        padded = jnp.pad(field, ((3, 3), (0, 0), (0, 0)))
        total = jnp.zeros_like(field)
        for offset in range(7):
            total = total + taps[offset] * padded[offset:offset + TIME]
        return total.reshape(TIME, TS, tile_cols, TS).transpose(2, 0, 1, 3)

    stacked = lax.map(one_row, jnp.arange(tile_rows, dtype=jnp.int32))
    return stacked.reshape(TILES, TIME, TS, TS)
```

```python
import functools

import jax
import jax.numpy as jnp
from jax import lax
from jax.experimental import pallas as pl
from jax.experimental.pallas import tpu as pltpu
from jax.sharding import PartitionSpec as P

TS = 512
REACH = 3
LATE = 1


def partner(me, m, n, sign):
    if n & (n - 1):
        return (me + sign * m + n) % n
    other, bit = me, 1
    while bit < n:
        if m & bit:
            other = other + bit * (1 - 2 * ((me // bit) % 2))
        bit *= 2
    return other


def exchange_kernel(groups, n, rows, width, sent, frames, stage, low, high, own, own_sem,
                    a_send, a_recv, up_send, up_recv, down_send, down_recv):
    steps = frames.shape[0]
    group, me = lax.axis_index("ta"), lax.axis_index("sa")
    across = frames.shape[3] // width
    order = sorted(range(1, n), key=lambda m: (bin(m >> 1).count("1"), m & 1, m))
    has_prev, has_next = group > 0, group < groups - 1

    def block_for(owner):
        row = pl.ds(pl.multiple_of((owner // across) * rows, 8), rows)
        if across == 1:
            return frames.at[:, 0, row, :]
        return frames.at[:, 0, row, pl.ds(pl.multiple_of((owner % across) * width, TS), width)]

    barrier = pltpu.get_barrier_semaphore()
    for m in order:
        pl.semaphore_signal(barrier, inc=1, device_id={"sa": partner(me, m, n, 1)})

    @pl.when(has_prev)
    def _():
        pl.semaphore_signal(barrier, inc=1, device_id={"ta": group - 1})

    @pl.when(has_next)
    def _():
        pl.semaphore_signal(barrier, inc=1, device_id={"ta": group + 1})

    def block_copy(m):
        return pltpu.make_async_remote_copy(
            src_ref=block_for(partner(me, m, n, 1)), dst_ref=stage.at[me],
            send_sem=a_send.at[m], recv_sem=a_recv.at[m], device_id={"sa": partner(me, m, n, 1)})

    def edge_copy(m, which):
        source = partner(me, m, n, -1)
        if m == 0:
            row = pl.ds(pl.multiple_of((me // across) * rows, 8), rows)
            col = pl.ds(pl.multiple_of((me % across) * width, TS), sent)
            tail = frames.at[pl.ds(steps - REACH, REACH), 0, row, col]
            head = frames.at[pl.ds(0, REACH), 0, row, col]
        else:
            tail = stage.at[source, pl.ds(steps - REACH, REACH), :, pl.ds(0, sent)]
            head = stage.at[source, pl.ds(0, REACH), :, pl.ds(0, sent)]
        if which == "up":
            return pltpu.make_async_remote_copy(
                src_ref=tail, dst_ref=low.at[source],
                send_sem=up_send.at[m], recv_sem=up_recv.at[m], device_id={"ta": group + 1})
        return pltpu.make_async_remote_copy(
            src_ref=head, dst_ref=high.at[source],
            send_sem=down_send.at[m], recv_sem=down_recv.at[m], device_id={"ta": group - 1})

    def send_edges(m):
        @pl.when(has_next)
        def _():
            edge_copy(m, "up").start()

        @pl.when(has_prev)
        def _():
            edge_copy(m, "down").start()

    load = pltpu.make_async_copy(block_for(me), own, own_sem.at[0])
    load.start()

    neighbours = jnp.where(has_prev, 1, 0) + jnp.where(has_next, 1, 0)
    pl.semaphore_wait(barrier, n - 1 + neighbours)

    send_edges(0)
    for m in order:
        block_copy(m).start()
    load.wait()
    store = pltpu.make_async_copy(own, stage.at[me], own_sem.at[1])
    store.start()
    for m in order:
        block_copy(m).wait_recv()
        send_edges(m)
    store.wait()
    for m in order:
        block_copy(m).wait_send()
    for m in [0] + order:
        @pl.when(has_next)
        def _():
            edge_copy(m, "up").wait_send()
            edge_copy(m, "down").wait_recv()

        @pl.when(has_prev)
        def _():
            edge_copy(m, "down").wait_send()
            edge_copy(m, "up").wait_recv()


def exchanged(frames, groups, n, rows, width, sent):
    steps = frames.shape[0]
    any_space = pl.BlockSpec(memory_space=pl.ANY)
    edge = jax.ShapeDtypeStruct((n, REACH, rows, sent), jnp.float32)
    dma = pltpu.SemaphoreType.DMA((n,))
    return pl.pallas_call(
        functools.partial(exchange_kernel, groups, n, rows, width, sent),
        out_shape=[jax.ShapeDtypeStruct((n, steps, rows, width), jnp.float32), edge, edge],
        in_specs=[any_space],
        out_specs=[any_space] * 3,
        scratch_shapes=[pltpu.VMEM((steps, rows, width), jnp.float32), pltpu.SemaphoreType.DMA((2,)),
                        dma, dma, dma, dma, dma, dma],
        compiler_params=pltpu.CompilerParams(collective_id=0, has_side_effects=True),
        name="exchange",
    )(frames)


def smooth_kernel(groups, taps, stage, low, high, *rest):
    out, woven = rest[-2:]
    n, steps, rows, cols = stage.shape
    group = lax.axis_index("ta")
    first, last = group == 0, group == groups - 1
    weights = [taps[j] for j in range(2 * REACH + 1)]

    for c in range(0, cols, 128):
        lanes = pl.ds(c, 128)

        def one_source(s, carry):
            for r in range(0, rows, 8):
                at = (pl.ds(r, 8), lanes)
                lo = [jnp.where(first, 0.0, low[(s, j) + at]) for j in range(REACH)]
                hi = [jnp.where(last, 0.0, high[(s, j) + at]) for j in range(REACH)]
                cells = lo + [stage[(s, t) + at] for t in range(steps)] + hi
                for t in range(steps):
                    total = weights[0] * cells[t]
                    for j in range(1, 2 * REACH + 1):
                        total = total + weights[j] * cells[t + j]
                    woven[t, pl.ds(r * n + s, 8, stride=n), :] = total
            return carry

        lax.fori_loop(0, n, one_source, 0)
        for t in range(steps):
            out[t, :, lanes] = woven[t]


def smoothed(taps, stage, low, high, groups, start, count, col_tiles, edge_start, owned, into=None):
    n, steps, rows, _ = stage.shape
    per_tile = TS // n
    height = min(per_tile, max(8, 256 // n))
    splits = per_tile // height

    def source_map(shift):
        return lambda k, h: (0, 0, ((k + start) // col_tiles) * splits + h, (k + start) % col_tiles - shift)

    specs = [
        pl.BlockSpec(memory_space=pltpu.SMEM),
        pl.BlockSpec((n, steps, height, TS), source_map(0)),
        pl.BlockSpec((n, REACH, height, TS), source_map(edge_start)),
        pl.BlockSpec((n, REACH, height, TS), source_map(edge_start)),
    ]
    operands = [taps, stage, low, high]
    if into is not None:
        specs.append(pl.BlockSpec(memory_space=pl.ANY))
        operands.append(into)
    moved = count * steps * TS * TS * 4
    return pl.pallas_call(
        functools.partial(smooth_kernel, groups),
        grid=(count, splits),
        out_shape=jax.ShapeDtypeStruct((owned, steps, TS, TS), jnp.float32),
        in_specs=specs,
        out_specs=pl.BlockSpec((None, steps, height * n, TS), lambda k, h: (k + start, 0, h, 0)),
        scratch_shapes=[pltpu.VMEM((steps, height * n, 128), jnp.float32)],
        input_output_aliases={} if into is None else {4: 0},
        compiler_params=pltpu.CompilerParams(vmem_limit_bytes=60 * 1024 * 1024),
        cost_estimate=pl.CostEstimate(flops=moved * 4, bytes_accessed=moved * 7 // 2, transcendentals=0),
        name="smooth",
    )(*operands)


def on_device(frames, taps):
    groups, n = lax.axis_size("ta"), lax.axis_size("sa")
    tile_rows, tile_cols = frames.shape[2] * n // TS, frames.shape[3] // TS
    owned = tile_rows * tile_cols // n
    col_tiles = min(owned, tile_cols)
    width = col_tiles * TS
    rows = max(1, owned // tile_cols) * (TS // n)
    late = LATE if owned == col_tiles and col_tiles > LATE else 0
    sent = width - late * TS
    stage, low, high = exchanged(frames, groups, n, rows, width, sent)
    if not late:
        return smoothed(taps, stage, low, high, groups, 0, owned, col_tiles, 0, owned)
    tail = lax.slice(stage, (0, stage.shape[1] - REACH, 0, sent), stage.shape)
    head = lax.slice(stage, (0, 0, 0, sent), (n, REACH, rows, width))
    late_low = lax.ppermute(tail, "ta", [(i, i + 1) for i in range(groups - 1)])
    late_high = lax.ppermute(head, "ta", [(i + 1, i) for i in range(groups - 1)])
    out = smoothed(taps, stage, low, high, groups, 0, owned - late, col_tiles, 0, owned)
    return smoothed(taps, stage, late_low, late_high, groups, owned - late, late, col_tiles, owned - late, owned, out)


def solution(mesh):
    placed = (P("ta", "sa", None, None), P())
    return jax.shard_map(
        on_device, mesh=mesh, in_specs=placed, out_specs=P("sa", "ta", None, None), check_vma=False
    )
```

```python
import functools

import jax
import jax.numpy as jnp
from jax import lax
from jax.experimental import pallas as pl
from jax.experimental.pallas import tpu as pltpu
from jax.sharding import PartitionSpec as P

TS = 512
REACH = 3
LATE = 1
LATE_SPAN = 256


def partner(me, m, n, sign):
    if n & (n - 1):
        return (me + sign * m + n) % n
    other, bit = me, 1
    while bit < n:
        if m & bit:
            other = other + bit * (1 - 2 * ((me // bit) % 2))
        bit *= 2
    return other


def exchange_kernel(groups, n, rows, width, sent, frames, *refs):
    late = sent < width
    stage, low, high = refs[:3]
    own, own_sem, a_send, a_recv, up_send, up_recv, down_send, down_recv = refs[-11 if late else -8:][:8]
    if late:
        head, tail = refs[3:5]
        late_cells, late_load, late_store = refs[-3:]
    steps = frames.shape[0]
    group, me = lax.axis_index("ta"), lax.axis_index("sa")
    across = frames.shape[3] // width
    order = sorted(range(1, n), key=lambda m: (bin(m >> 1).count("1"), m & 1, m))
    has_prev, has_next = group > 0, group < groups - 1

    def block_for(owner):
        row = pl.ds(pl.multiple_of((owner // across) * rows, 8), rows)
        if across == 1:
            return frames.at[:, 0, row, :]
        return frames.at[:, 0, row, pl.ds(pl.multiple_of((owner % across) * width, TS), width)]

    barrier = pltpu.get_barrier_semaphore()
    for m in order:
        pl.semaphore_signal(barrier, inc=1, device_id={"sa": partner(me, m, n, 1)})

    @pl.when(has_prev)
    def _():
        pl.semaphore_signal(barrier, inc=1, device_id={"ta": group - 1})

    @pl.when(has_next)
    def _():
        pl.semaphore_signal(barrier, inc=1, device_id={"ta": group + 1})

    def block_copy(m):
        return pltpu.make_async_remote_copy(
            src_ref=block_for(partner(me, m, n, 1)), dst_ref=stage.at[me],
            send_sem=a_send.at[m], recv_sem=a_recv.at[m], device_id={"sa": partner(me, m, n, 1)})

    def edge_copy(m, which):
        source = partner(me, m, n, -1)
        if m == 0:
            row = pl.ds(pl.multiple_of((me // across) * rows, 8), rows)
            col = pl.ds(pl.multiple_of((me % across) * width, TS), sent)
            ending = frames.at[pl.ds(steps - REACH, REACH), 0, row, col]
            opening = frames.at[pl.ds(0, REACH), 0, row, col]
        else:
            ending = stage.at[source, pl.ds(steps - REACH, REACH), :, pl.ds(0, sent)]
            opening = stage.at[source, pl.ds(0, REACH), :, pl.ds(0, sent)]
        if which == "up":
            return pltpu.make_async_remote_copy(
                src_ref=ending, dst_ref=low.at[source],
                send_sem=up_send.at[m], recv_sem=up_recv.at[m], device_id={"ta": group + 1})
        return pltpu.make_async_remote_copy(
            src_ref=opening, dst_ref=high.at[source],
            send_sem=down_send.at[m], recv_sem=down_recv.at[m], device_id={"ta": group - 1})

    def send_edges(m):
        @pl.when(has_next)
        def _():
            edge_copy(m, "up").start()

        @pl.when(has_prev)
        def _():
            edge_copy(m, "down").start()

    def late_copies(m):
        source = partner(me, m, n, -1)
        return (
            pltpu.make_async_copy(late_cells.at[m, pl.ds(steps - REACH, REACH)], tail.at[source], late_store.at[0, m]),
            pltpu.make_async_copy(late_cells.at[m, pl.ds(0, REACH)], head.at[source], late_store.at[1, m]),
        )

    def take_late(m):
        if m == 0:
            row = pl.ds(pl.multiple_of((me // across) * rows, 8), rows)
            col = pl.ds(pl.multiple_of((me % across) * width + sent, TS), width - sent)
            cells = frames.at[:, 0, row, col]
        else:
            cells = stage.at[partner(me, m, n, -1), :, :, pl.ds(sent, width - sent)]
        taken = pltpu.make_async_copy(cells, late_cells.at[m], late_load.at[m])
        taken.start()
        taken.wait()
        for put in late_copies(m):
            put.start()

    load = pltpu.make_async_copy(block_for(me), own, own_sem.at[0])
    load.start()

    neighbours = jnp.where(has_prev, 1, 0) + jnp.where(has_next, 1, 0)
    pl.semaphore_wait(barrier, n - 1 + neighbours)

    send_edges(0)
    for m in order:
        block_copy(m).start()
    load.wait()
    store = pltpu.make_async_copy(own, stage.at[me], own_sem.at[1])
    store.start()
    if late:
        take_late(0)
    for m in order:
        block_copy(m).wait_recv()
        send_edges(m)
        if late:
            take_late(m)
    store.wait()
    if late:
        for m in [0] + order:
            for put in late_copies(m):
                put.wait()
    for m in order:
        block_copy(m).wait_send()
    for m in [0] + order:
        @pl.when(has_next)
        def _():
            edge_copy(m, "up").wait_send()
            edge_copy(m, "down").wait_recv()

        @pl.when(has_prev)
        def _():
            edge_copy(m, "down").wait_send()
            edge_copy(m, "up").wait_recv()


def exchanged(frames, groups, n, rows, width, sent):
    steps = frames.shape[0]
    any_space = pl.BlockSpec(memory_space=pl.ANY)
    edge = jax.ShapeDtypeStruct((n, REACH, rows, sent), jnp.float32)
    dma = pltpu.SemaphoreType.DMA((n,))
    shapes = [jax.ShapeDtypeStruct((n, steps, rows, width), jnp.float32), edge, edge]
    scratch = [pltpu.VMEM((steps, rows, width), jnp.float32), pltpu.SemaphoreType.DMA((2,))] + [dma] * 6
    if sent < width:
        shapes += [jax.ShapeDtypeStruct((n, REACH, rows, width - sent), jnp.float32)] * 2
        scratch += [pltpu.VMEM((n, steps, rows, width - sent), jnp.float32), dma, pltpu.SemaphoreType.DMA((2, n))]
    return pl.pallas_call(
        functools.partial(exchange_kernel, groups, n, rows, width, sent),
        out_shape=shapes,
        in_specs=[any_space],
        out_specs=[any_space] * len(shapes),
        scratch_shapes=scratch,
        compiler_params=pltpu.CompilerParams(collective_id=0, has_side_effects=True),
        name="exchange",
    )(frames)


def smooth_kernel(groups, taps, stage, low, high, *rest):
    out, woven = rest[-2:]
    n, steps, rows, cols = stage.shape
    group = lax.axis_index("ta")
    first, last = group == 0, group == groups - 1
    weights = [taps[j] for j in range(2 * REACH + 1)]

    for c in range(0, cols, 128):
        lanes = pl.ds(c, 128)

        def one_source(s, carry):
            for r in range(0, rows, 8):
                at = (pl.ds(r, 8), lanes)
                lo = [jnp.where(first, 0.0, low[(s, j) + at]) for j in range(REACH)]
                hi = [jnp.where(last, 0.0, high[(s, j) + at]) for j in range(REACH)]
                cells = lo + [stage[(s, t) + at] for t in range(steps)] + hi
                for t in range(steps):
                    total = weights[0] * cells[t]
                    for j in range(1, 2 * REACH + 1):
                        total = total + weights[j] * cells[t + j]
                    woven[t, pl.ds(r * n + s, 8, stride=n), :] = total
            return carry

        lax.fori_loop(0, n, one_source, 0)
        for t in range(steps):
            out[t, :, lanes] = woven[t]


def smoothed(taps, stage, low, high, groups, start, count, col_tiles, edge_start, owned, span, into=None):
    n, steps, rows, _ = stage.shape
    per_tile = TS // n
    height = min(per_tile, max(8, span // n))
    splits = per_tile // height

    def source_map(shift):
        return lambda k, h: (0, 0, ((k + start) // col_tiles) * splits + h, (k + start) % col_tiles - shift)

    specs = [
        pl.BlockSpec(memory_space=pltpu.SMEM),
        pl.BlockSpec((n, steps, height, TS), source_map(0)),
        pl.BlockSpec((n, REACH, height, TS), source_map(edge_start)),
        pl.BlockSpec((n, REACH, height, TS), source_map(edge_start)),
    ]
    operands = [taps, stage, low, high]
    if into is not None:
        specs.append(pl.BlockSpec(memory_space=pl.ANY))
        operands.append(into)
    moved = count * steps * TS * TS * 4
    return pl.pallas_call(
        functools.partial(smooth_kernel, groups),
        grid=(count, splits),
        out_shape=jax.ShapeDtypeStruct((owned, steps, TS, TS), jnp.float32),
        in_specs=specs,
        out_specs=pl.BlockSpec((None, steps, height * n, TS), lambda k, h: (k + start, 0, h, 0)),
        scratch_shapes=[pltpu.VMEM((steps, height * n, 128), jnp.float32)],
        input_output_aliases={} if into is None else {4: 0},
        compiler_params=pltpu.CompilerParams(vmem_limit_bytes=60 * 1024 * 1024),
        cost_estimate=pl.CostEstimate(flops=moved * 4, bytes_accessed=moved * 7 // 2, transcendentals=0),
        name="smooth",
    )(*operands)


def on_device(frames, taps):
    groups, n = lax.axis_size("ta"), lax.axis_size("sa")
    tile_rows, tile_cols = frames.shape[2] * n // TS, frames.shape[3] // TS
    owned = tile_rows * tile_cols // n
    col_tiles = min(owned, tile_cols)
    width = col_tiles * TS
    rows = max(1, owned // tile_cols) * (TS // n)
    late = LATE if owned == col_tiles and col_tiles > LATE else 0
    sent = width - late * TS
    stage, low, high, *edges = exchanged(frames, groups, n, rows, width, sent)
    if not late:
        return smoothed(taps, stage, low, high, groups, 0, owned, col_tiles, 0, owned, 256)
    head, tail = edges
    late_low = lax.ppermute(tail, "ta", [(i, i + 1) for i in range(groups - 1)])
    late_high = lax.ppermute(head, "ta", [(i + 1, i) for i in range(groups - 1)])
    out = smoothed(taps, stage, low, high, groups, 0, owned - late, col_tiles, 0, owned, 256)
    return smoothed(taps, stage, late_low, late_high, groups, owned - late, late, col_tiles, owned - late, owned, LATE_SPAN, out)


def solution(mesh):
    placed = (P("ta", "sa", None, None), P())
    return jax.shard_map(
        on_device, mesh=mesh, in_specs=placed, out_specs=P("sa", "ta", None, None), check_vma=False
    )
```
